32 devices in a mesh: blk: 32 (over z, y, x, core).
Axes of the slice: x: 2, y: 2, z: 4, core: 2. Of those that a mesh axis runs over, the one named last changes fastest.
Arguments:
- tiles: float32 [128, 3, 256, 256], P('blk'), may hold values from -0.109375 to 0.109375
- offsets: int32 [128, 3], P('blk'), may hold values from -2 to 2, as said below
- start: float32 [32768, 128], P('blk'), may hold values from -6 to 6
Outputs:
- grams: float32 [2, 8, 8, 128], replicated
- final: float32 [32768, 128], P('blk')
The draws below stay inside these ranges and needn't reach their ends.
Inputs may be any that keep to these rules, and one draw needn't show every extreme that they name: The 3 offsets of a block row are all different.
All inputs are finite; a program needn't handle non-finite values.
Results may differ from the reference program's by a relative error of at most 0.00018.
Values sent between devices are 32-bit elements; how exact they have to be, the bound alone decides.
A program may use at most 128 MiB of HBM per device.

```python
import jax
import jax.numpy as jnp
from jax import lax

TILE = 256
SLOTS = 3
REACH = 2
PROBES = 128
OUTER = 2
DEPTH = 4
NBLK = 128
NROWS = 32768


def draw_offsets(key, part):
    width = 2 * REACH + 1
    scores = jax.random.randint(key, (NBLK, width), 0, 1 << 20) * width + jnp.arange(width, dtype=jnp.int32)
    order = jnp.argsort(scores, axis=1)
    return (order[:, :SLOTS] - REACH).astype(jnp.int32)


def shard_levels(own_key, extent, cuts, low, largest):
    gain = 1.0
    for dim, blocks in cuts:
        steps = jax.random.uniform(jax.random.fold_in(jax.random.fold_in(own_key, 6), dim), (blocks,), jnp.float32, low / len(cuts), largest / len(cuts))
        gain = gain * jnp.repeat(jnp.exp(steps), extent[dim] // blocks).reshape((-1,) + (1,) * (len(extent) - 1 - dim))
    return gain


def normal_values(key, dims, deviation, most, pieces=(), kind=jnp.bfloat16):
    entries = jax.random.normal(key, dims, jnp.float32) * deviation
    if len(pieces) > 0:
        entries = shard_levels(key, dims, pieces, -0.22, 0.18) * entries
    return jnp.clip(entries, min=-most, max=most).astype(kind)


def setup_inputs(seed: int = 0) -> dict:
    key_list = jax.random.split(jax.random.key(seed), 4)
    return {
        "tiles": normal_values(key_list[0], (NBLK, SLOTS, TILE, TILE), (4 * SLOTS * TILE) ** -0.5, 0.109375, ((0, 32),), jnp.float32),
        "offsets": draw_offsets(jax.random.fold_in(key_list[3], 71), 0),
        "start": normal_values(key_list[2], (NROWS, PROBES), 1.0, 6.0, ((0, 32),), jnp.float32),
    }


def forward_all(tiles, offsets, field):
    nblk = tiles.shape[0]
    blocks = field.reshape(nblk, TILE, field.shape[1])
    index = (jnp.arange(nblk, dtype=jnp.int32)[:, None] + offsets) % nblk
    picked = blocks[index]
    image = jnp.einsum('rkab,rkbp->rap', tiles, picked, precision=lax.Precision.HIGHEST)
    return image.reshape(field.shape)

def adjoint_all(tiles, offsets, field):
    nblk = tiles.shape[0]
    probes = field.shape[1]
    blocks = field.reshape(nblk, TILE, probes)
    parts = jnp.einsum('rkab,rap->rkbp', tiles, blocks, precision=lax.Precision.HIGHEST)
    target = ((jnp.arange(nblk, dtype=jnp.int32)[:, None] + offsets) % nblk).reshape(-1)
    total = jnp.zeros_like(blocks).at[target].add(parts.reshape(-1, TILE, probes))
    return total.reshape(field.shape)

def reference(tiles, offsets, start):
    current = start
    grams = []
    for outer in range(OUTER):
        basis_p = [current]
        basis_q = []
        for depth in range(DEPTH):
            image = forward_all(tiles, offsets, basis_p[-1])
            basis_q.append(image)
            basis_p.append(adjoint_all(tiles, offsets, image))
        stack = jnp.stack(basis_p[:DEPTH] + basis_q)
        gram = jnp.einsum('arp,brp->abp', stack, stack, precision=lax.Precision.HIGHEST) / NROWS
        grams.append(gram)
        current = basis_p[DEPTH] / jnp.sqrt(gram[-1, -1] + 0.25)
    return (jnp.stack(grams), current)
```

```python
import functools

import jax
import jax.numpy as jnp
from jax import lax
from jax.experimental import pallas as pl
from jax.experimental.pallas import tpu as pltpu
from jax.sharding import PartitionSpec as P

REACH = 2
OUTER = 2
DEPTH = 4
MESH = pl.DeviceIdType.MESH
F32 = jnp.float32
BF16 = jnp.bfloat16


def halves(x):
    high = x.astype(BF16)
    return high, (x - high.astype(F32)).astype(BF16)


def kernel(
    n,
    levels,
    total_rows,
    off_ref,
    tiles_hbm,
    start_hbm,
    gram_ref,
    final_ref,
    raw,
    fwd,
    adj,
    basis,
    field,
    image,
    parts,
    halo_l,
    halo_r,
    give_l,
    give_r,
    part_l,
    part_r,
    gram,
    sums,
    heard,
    load_sem,
    send_sem,
    recv_sem,
    sum_send,
    sum_recv,
):
    nblk, slots, tile, _ = raw.shape
    probes = basis.shape[2]
    edge = REACH * tile
    me = lax.axis_index("blk")
    left, right = lax.rem(me + n - 1, n), lax.rem(me + 1, n)
    partners = []
    for b in range(levels):
        s = 1 << b
        partners.append(me + s * (1 - 2 * lax.rem(me // s, 2)))

    load_start = pltpu.make_async_copy(start_hbm, basis.at[0], load_sem.at[0])
    load_start.start()
    load_tiles = pltpu.make_async_copy(tiles_hbm, raw, load_sem.at[1])
    load_tiles.start()

    barrier = pltpu.get_barrier_semaphore()
    for other in [left, right] + partners:
        pl.semaphore_signal(barrier, inc=1, device_id=(other,), device_id_type=MESH)

    def remote(src, dst, k, device):
        return pltpu.make_async_remote_copy(
            src_ref=src,
            dst_ref=dst,
            send_sem=send_sem.at[k],
            recv_sem=recv_sem.at[k],
            device_id=(device,),
            device_id_type=MESH,
        )

    def edges(t):
        return (
            remote(basis.at[t, pl.ds(0, edge)], halo_r, 0, left),
            remote(basis.at[t, pl.ds(nblk * tile - edge, edge)], halo_l, 1, right),
        )

    def give():
        return remote(give_l, part_r, 2, left), remote(give_r, part_l, 3, right)

    def sum_step(outer, b):
        k = outer * levels + b
        return pltpu.make_async_remote_copy(
            src_ref=sums.at[outer * (levels + 1) + b],
            dst_ref=heard.at[k],
            send_sem=sum_send.at[k],
            recv_sem=sum_recv.at[k],
            device_id=(partners[b],),
            device_id_type=MESH,
        )

    where = [[i + REACH + off_ref[i, k] for k in range(slots)] for i in range(nblk)]
    source = {}
    for i in range(nblk):
        for d in range(-REACH, REACH + 1):
            index = nblk * slots
            for k in range(slots):
                index = jnp.where(off_ref[i, k] == d, i * slots + k, index)
            source[i, d] = index

    gram[...] = jnp.zeros_like(gram)
    parts[nblk * slots] = jnp.zeros((tile, probes), F32)

    load_start.wait()
    pl.semaphore_wait(barrier, 2 + levels)
    for copy in edges(0):
        copy.start()
    load_tiles.wait()

    def prepare(i, carry):
        for k in range(slots):
            value = raw[i, k]
            high, low = halves(value)
            fwd[i, pl.ds(0, tile), pl.ds(k * tile, tile)] = high
            fwd[i, pl.ds(tile, tile), pl.ds(k * tile, tile)] = low
            high, low = halves(value.T)
            adj[i, pl.ds(2 * k * tile, tile), :] = high
            adj[i, pl.ds((2 * k + 1) * tile, tile), :] = low
        return carry

    lax.fori_loop(0, nblk, prepare, 0)

    def keep(ref, i, value):
        high, low = halves(value)
        ref[i, :, pl.ds(0, probes)] = high
        ref[i, :, pl.ds(probes, probes)] = low

    def joined(r, base):
        top = r[base : base + tile]
        low = r[base + tile : base + 2 * tile]
        return (top[:, :probes] + top[:, probes:]) + (low[:, :probes] + low[:, probes:])

    def gram_rows(t):
        def one(u, carry):
            prod = basis[t] * basis[u]
            s = jnp.sum(prod.reshape(-1, 8, probes), axis=0)
            gram[pl.ds(t * 2 * DEPTH + u, 1), :] = jnp.sum(s, axis=0, keepdims=True)
            return carry

        lax.fori_loop(0, t + 1, one, 0)

    def pair(outer, j, last):
        t = 2 * j
        for i in range(nblk):
            keep(field, i + REACH, basis[t, pl.ds(i * tile, tile), :])
        gram_rows(t)
        for copy in edges(t):
            copy.wait()
        for h in range(REACH):
            keep(field, h, halo_l[pl.ds(h * tile, tile), :])
            keep(field, nblk + REACH + h, halo_r[pl.ds(h * tile, tile), :])
        for i in range(nblk):
            rhs = jnp.concatenate([field[where[i][k]] for k in range(slots)], axis=0)
            q = joined(jnp.dot(fwd[i], rhs, preferred_element_type=F32), 0)
            basis[t + 1, pl.ds(i * tile, tile), :] = q
            keep(image, i, q)
        if last:
            gram_rows(t + 1)
            sums[outer * (levels + 1)] = gram[...]
            sum_step(outer, 0).start()

        def spread(i):
            r = jnp.dot(adj[i], image[i], preferred_element_type=F32)
            for k in range(slots):
                parts[i * slots + k] = joined(r, 2 * k * tile)

        def gathered(target):
            total = None
            for i in range(nblk):
                if abs(target - i) <= REACH:
                    term = parts[source[i, target - i]]
                    total = term if total is None else total + term
            return total

        done = []
        for i in range(min(REACH, nblk)):
            spread(i)
            done.append(i)
        for h in range(REACH):
            give_l[pl.ds(h * tile, tile), :] = gathered(h - REACH)
        to_left, to_right = give()
        to_left.start()
        for i in range(nblk):
            if i not in done:
                spread(i)
        for h in range(REACH):
            give_r[pl.ds(h * tile, tile), :] = gathered(nblk + h)
        to_right.start()
        for i in range(nblk):
            basis[t + 2, pl.ds(i * tile, tile), :] = gathered(i)
        if last:
            for b in range(levels):
                sum_step(outer, b).wait()
                k = outer * (levels + 1) + b
                sums[k + 1] = sums[k] + heard[outer * levels + b]
                if b + 1 < levels:
                    sum_step(outer, b + 1).start()
        else:
            gram_rows(t + 1)
        to_left.wait()
        to_right.wait()
        basis[t + 2, pl.ds(0, edge), :] += part_l[...]
        basis[t + 2, pl.ds(nblk * tile - edge, edge), :] += part_r[...]

    def outer_step(outer, carry):
        def inner(j, c):
            pair(outer, j, False)
            for copy in edges(2 * j + 2):
                copy.start()
            return c

        lax.fori_loop(0, DEPTH - 1, inner, 0)
        pair(outer, DEPTH - 1, True)
        total = outer * (levels + 1) + levels
        size = 2 * DEPTH
        corner = sums[total, pl.ds(size * size - 1, 1), :] / total_rows
        scale = 1.0 / jnp.sqrt(corner + 0.25)
        basis[0] = basis[size] * scale

        @pl.when(outer < OUTER - 1)
        def _():
            for copy in edges(0):
                copy.start()

        when = [2 * a for a in range(DEPTH)] + [2 * a + 1 for a in range(DEPTH)]
        for a in range(size):
            for b in range(size):
                row = max(when[a], when[b]) * size + min(when[a], when[b])
                gram_ref[outer, pl.ds(a * size + b, 1), :] = (
                    sums[total, pl.ds(row, 1), :] / total_rows
                )
        return carry

    lax.fori_loop(0, OUTER, outer_step, 0)
    final_ref[...] = basis[0]


def on_device(tiles, offsets, start):
    n = lax.axis_size("blk")
    levels = n.bit_length() - 1
    assert n == 1 << levels
    nblk, slots, tile, _ = tiles.shape
    rows, probes = start.shape
    edge = REACH * tile
    size = 2 * DEPTH
    dma = pltpu.SemaphoreType.DMA
    grams, final = pl.pallas_call(
        functools.partial(kernel, n, levels, float(rows * n)),
        out_shape=(
            jax.ShapeDtypeStruct((OUTER, size * size, probes), F32),
            jax.ShapeDtypeStruct((rows, probes), F32),
        ),
        in_specs=[
            pl.BlockSpec(memory_space=pltpu.SMEM),
            pl.BlockSpec(memory_space=pl.ANY),
            pl.BlockSpec(memory_space=pl.ANY),
        ],
        out_specs=(pl.BlockSpec(memory_space=pltpu.VMEM), pl.BlockSpec(memory_space=pltpu.VMEM)),
        scratch_shapes=[
            pltpu.VMEM(tiles.shape, F32),
            pltpu.VMEM((nblk, 2 * tile, slots * tile), BF16),
            pltpu.VMEM((nblk, 2 * slots * tile, tile), BF16),
            pltpu.VMEM((size + 1, rows, probes), F32),
            pltpu.VMEM((nblk + 2 * REACH, tile, 2 * probes), BF16),
            pltpu.VMEM((nblk, tile, 2 * probes), BF16),
            pltpu.VMEM((nblk * slots + 1, tile, probes), F32),
        ]
        + [pltpu.VMEM((edge, probes), F32)] * 6
        + [
            pltpu.VMEM((size * size, probes), F32),
            pltpu.VMEM((OUTER * (levels + 1), size * size, probes), F32),
            pltpu.VMEM((OUTER * levels, size * size, probes), F32),
            dma((2,)),
            dma((4,)),
            dma((4,)),
            dma((OUTER * levels,)),
            dma((OUTER * levels,)),
        ],
        compiler_params=pltpu.CompilerParams(collective_id=0, has_side_effects=True),
    )(offsets, tiles, start)
    return grams.reshape(OUTER, size, size, probes), final


def solution(mesh):
    placed = (P("blk", None, None, None), P("blk", None), P("blk", None))
    return jax.shard_map(
        on_device, mesh=mesh, in_specs=placed, out_specs=(P(), P("blk", None)), check_vma=False
    )
```

```python
import functools

import jax
import jax.numpy as jnp
from jax import lax
from jax.experimental import pallas as pl
from jax.experimental.pallas import tpu as pltpu
from jax.sharding import PartitionSpec as P

REACH = 2
OUTER = 2
DEPTH = 4
MESH = pl.DeviceIdType.MESH
F32 = jnp.float32
BF16 = jnp.bfloat16


def halves(x):
    high = x.astype(BF16)
    return high, (x - high.astype(F32)).astype(BF16)


def kernel(
    n,
    levels,
    total_rows,
    off_ref,
    tiles_hbm,
    start_hbm,
    gram_ref,
    final_ref,
    raw,
    fwd,
    adj,
    basis,
    field,
    image,
    parts,
    halo,
    give,
    got,
    gram,
    sums,
    heard,
    load_sem,
    send_sem,
    recv_sem,
    sum_send,
    sum_recv,
):
    nblk, slots, tile, _ = raw.shape
    probes = basis.shape[3]
    me = lax.axis_index("blk")
    slow = lax.rem(me, 2)
    fast = 1 - slow
    left, right = lax.rem(me + n - 1, n), lax.rem(me + 1, n)
    partners = []
    for b in range(levels):
        s = 1 << b
        partners.append(me + s * (1 - 2 * lax.rem(me // s, 2)))

    load_start = pltpu.make_async_copy(start_hbm, basis.at[0], load_sem.at[0])
    load_start.start()
    load_tiles = pltpu.make_async_copy(tiles_hbm, raw, load_sem.at[1])
    load_tiles.start()

    barrier = pltpu.get_barrier_semaphore()
    for other in [left, right] + partners:
        pl.semaphore_signal(barrier, inc=1, device_id=(other,), device_id_type=MESH)

    def block(side, k):
        return side * (nblk - 1) + k * (1 - 2 * side)

    def beyond(side, k):
        return side * (nblk + 1 + 2 * k) - 1 - k

    def remote(src, dst, here, there, side):
        return pltpu.make_async_remote_copy(
            src_ref=src,
            dst_ref=dst,
            send_sem=send_sem.at[here],
            recv_sem=recv_sem.at[there],
            device_id=(lax.rem(me + n - 1 + 2 * side, n),),
            device_id_type=MESH,
        )

    def send_p(t, side, k):
        there = (1 - side) * REACH + k
        remote(basis.at[t, block(side, k)], halo.at[there], side * REACH + k, there, side).start()

    def wait_p(t, side, k):
        here = side * REACH + k
        remote(basis.at[t, block(side, k)], halo.at[here], here, here, side).wait()

    def send_part(side, k):
        here, there = side * REACH + k, (1 - side) * REACH + k
        more = 2 * REACH
        remote(give.at[here], got.at[there], more + here, more + there, side).start()

    def wait_part(side, k):
        here = side * REACH + k
        sem = 2 * REACH + here
        remote(give.at[here], got.at[here], sem, sem, side).wait()

    def sum_step(outer, b):
        k = outer * levels + b
        return pltpu.make_async_remote_copy(
            src_ref=sums.at[outer * (levels + 1) + b],
            dst_ref=heard.at[k],
            send_sem=sum_send.at[k],
            recv_sem=sum_recv.at[k],
            device_id=(partners[b],),
            device_id_type=MESH,
        )

    def source(i, d):
        index = nblk * slots
        for k in range(slots):
            index = jnp.where(off_ref[i, k] == d, i * slots + k, index)
        return index

    gram[...] = jnp.zeros_like(gram)
    parts[nblk * slots] = jnp.zeros((tile, probes), F32)

    load_start.wait()
    pl.semaphore_wait(barrier, 2 + levels)
    for k in range(REACH):
        send_p(0, slow, k)
        send_p(0, fast, k)
    load_tiles.wait()

    def prepare(i, carry):
        for k in range(slots):
            value = raw[i, k]
            high, low = halves(value)
            fwd[i, pl.ds(0, tile), pl.ds(k * tile, tile)] = high
            fwd[i, pl.ds(tile, tile), pl.ds(k * tile, tile)] = low
            high, low = halves(value.T)
            adj[i, pl.ds(2 * k * tile, tile), :] = high
            adj[i, pl.ds((2 * k + 1) * tile, tile), :] = low
        return carry

    lax.fori_loop(0, nblk, prepare, 0)

    def keep(ref, i, value):
        high, low = halves(value)
        ref[i, :, pl.ds(0, probes)] = high
        ref[i, :, pl.ds(probes, probes)] = low

    def joined(r, base):
        top = r[base : base + tile]
        low = r[base + tile : base + 2 * tile]
        return (top[:, :probes] + top[:, probes:]) + (low[:, :probes] + low[:, probes:])

    def gram_rows(t):
        def one(u, carry):
            prod = (basis[t] * basis[u]).reshape(-1, probes)
            s = jnp.sum(prod.reshape(-1, 8, probes), axis=0)
            gram[pl.ds(t * 2 * DEPTH + u, 1), :] = jnp.sum(s, axis=0, keepdims=True)
            return carry

        lax.fori_loop(0, t + 1, one, 0)

    def forward(t, i):
        rhs = jnp.concatenate([field[i + REACH + off_ref[i, k]] for k in range(slots)], axis=0)
        q = joined(jnp.dot(fwd[i], rhs, preferred_element_type=F32), 0)
        basis[t + 1, i] = q
        keep(image, i, q)
        r = jnp.dot(adj[i], image[i], preferred_element_type=F32)
        for k in range(slots):
            parts[i * slots + k] = joined(r, 2 * k * tile)

    def arrive(t, side, k):
        wait_p(t, side, k)
        keep(field, beyond(side, k) + REACH, halo[side * REACH + k])

    def hand_over(side):
        for k in range(REACH):
            total = None
            for r in range(REACH - k):
                term = parts[source(block(side, r), (2 * side - 1) * (r + 1 + k))]
                total = term if total is None else total + term
            give[side * REACH + k] = total
            send_part(side, k)

    def gathered(target):
        total = None
        for i in range(nblk):
            if abs(target - i) <= REACH:
                term = parts[source(i, target - i)]
                total = term if total is None else total + term
        return total

    def take(t, side, k, last):
        wait_part(side, k)
        basis[t, block(side, k)] += got[side * REACH + k]
        if not last:
            send_p(t, side, k)

    def pair(outer, j, last):
        t = 2 * j
        for i in range(nblk):
            keep(field, i + REACH, basis[t, i])
        gram_rows(t)
        for k in range(REACH):
            arrive(t, fast, k)
        for i in range(REACH, nblk - REACH):
            forward(t, i)
        for k in reversed(range(REACH)):
            forward(t, block(fast, k))
        hand_over(fast)
        for k in range(REACH):
            arrive(t, slow, k)
            forward(t, block(slow, REACH - 1 - k))
        hand_over(slow)
        if last:
            gram_rows(t + 1)
            sums[outer * (levels + 1)] = gram[...]
            sum_step(outer, 0).start()
        for i in range(nblk):
            basis[t + 2, i] = gathered(i)
        for k in range(REACH):
            take(t + 2, fast, k, last)
        if last:
            for b in range(levels):
                sum_step(outer, b).wait()
                k = outer * (levels + 1) + b
                sums[k + 1] = sums[k] + heard[outer * levels + b]
                if b + 1 < levels:
                    sum_step(outer, b + 1).start()
        else:
            gram_rows(t + 1)
        for k in range(REACH):
            take(t + 2, slow, k, last)

    def outer_step(outer, carry):
        def inner(j, c):
            pair(outer, j, False)
            return c

        lax.fori_loop(0, DEPTH - 1, inner, 0)
        pair(outer, DEPTH - 1, True)
        total = outer * (levels + 1) + levels
        size = 2 * DEPTH
        corner = sums[total, pl.ds(size * size - 1, 1), :] / total_rows
        scale = 1.0 / jnp.sqrt(corner + 0.25)
        basis[0] = basis[size] * scale[None]

        @pl.when(outer < OUTER - 1)
        def _():
            for k in range(REACH):
                send_p(0, slow, k)
                send_p(0, fast, k)

        when = [2 * a for a in range(DEPTH)] + [2 * a + 1 for a in range(DEPTH)]
        for a in range(size):
            for b in range(size):
                row = max(when[a], when[b]) * size + min(when[a], when[b])
                gram_ref[outer, pl.ds(a * size + b, 1), :] = (
                    sums[total, pl.ds(row, 1), :] / total_rows
                )
        return carry

    lax.fori_loop(0, OUTER, outer_step, 0)
    final_ref[...] = basis[0]


def on_device(tiles, offsets, start):
    n = lax.axis_size("blk")
    levels = n.bit_length() - 1
    assert n == 1 << levels
    nblk, slots, tile, _ = tiles.shape
    rows, probes = start.shape
    assert nblk >= 2 * REACH
    size = 2 * DEPTH
    dma = pltpu.SemaphoreType.DMA
    grams, final = pl.pallas_call(
        functools.partial(kernel, n, levels, float(rows * n)),
        out_shape=(
            jax.ShapeDtypeStruct((OUTER, size * size, probes), F32),
            jax.ShapeDtypeStruct((nblk, tile, probes), F32),
        ),
        in_specs=[
            pl.BlockSpec(memory_space=pltpu.SMEM),
            pl.BlockSpec(memory_space=pl.ANY),
            pl.BlockSpec(memory_space=pl.ANY),
        ],
        out_specs=(pl.BlockSpec(memory_space=pltpu.VMEM), pl.BlockSpec(memory_space=pltpu.VMEM)),
        scratch_shapes=[
            pltpu.VMEM(tiles.shape, F32),
            pltpu.VMEM((nblk, 2 * tile, slots * tile), BF16),
            pltpu.VMEM((nblk, 2 * slots * tile, tile), BF16),
            pltpu.VMEM((size + 1, nblk, tile, probes), F32),
            pltpu.VMEM((nblk + 2 * REACH, tile, 2 * probes), BF16),
            pltpu.VMEM((nblk, tile, 2 * probes), BF16),
            pltpu.VMEM((nblk * slots + 1, tile, probes), F32),
        ]
        + [pltpu.VMEM((2 * REACH, tile, probes), F32)] * 3
        + [
            pltpu.VMEM((size * size, probes), F32),
            pltpu.VMEM((OUTER * (levels + 1), size * size, probes), F32),
            pltpu.VMEM((OUTER * levels, size * size, probes), F32),
            dma((2,)),
            dma((4 * REACH,)),
            dma((4 * REACH,)),
            dma((OUTER * levels,)),
            dma((OUTER * levels,)),
        ],
        compiler_params=pltpu.CompilerParams(collective_id=0, has_side_effects=True),
    )(offsets, tiles, start.reshape(nblk, tile, probes))
    return grams.reshape(OUTER, size, size, probes), final.reshape(rows, probes)


def solution(mesh):
    placed = (P("blk", None, None, None), P("blk", None), P("blk", None))
    return jax.shard_map(
        on_device, mesh=mesh, in_specs=placed, out_specs=(P(), P("blk", None)), check_vma=False
    )
```

```python
import functools

import jax
import jax.numpy as jnp
from jax import lax
from jax.experimental import pallas as pl
from jax.experimental.pallas import tpu as pltpu
from jax.sharding import PartitionSpec as P

REACH = 2
OUTER = 2
DEPTH = 4
SPLIT = 2
MESH = pl.DeviceIdType.MESH
F32 = jnp.float32
BF16 = jnp.bfloat16


def halves(x):
    high = x.astype(BF16)
    return high, (x - high.astype(F32)).astype(BF16)


def kernel(
    n,
    levels,
    total_rows,
    off_ref,
    tiles_hbm,
    start_hbm,
    gram_ref,
    final_ref,
    raw,
    fwd,
    adj,
    basis,
    field,
    image,
    parts,
    halo,
    give,
    got,
    gram,
    sums,
    heard,
    load_sem,
    send_sem,
    recv_sem,
    sum_send,
    sum_recv,
):
    nblk, slots, tile, _ = raw.shape
    probes = basis.shape[3]
    me = lax.axis_index("blk")
    slow = lax.rem(me, 2)
    fast = 1 - slow
    left, right = lax.rem(me + n - 1, n), lax.rem(me + 1, n)
    partners = []
    for b in range(levels):
        s = 1 << b
        partners.append(me + s * (1 - 2 * lax.rem(me // s, 2)))

    load_start = pltpu.make_async_copy(start_hbm, basis.at[0], load_sem.at[0])
    load_start.start()
    load_tiles = pltpu.make_async_copy(tiles_hbm, raw, load_sem.at[1])
    load_tiles.start()

    barrier = pltpu.get_barrier_semaphore()
    for other in [left, right] + partners:
        pl.semaphore_signal(barrier, inc=1, device_id=(other,), device_id_type=MESH)

    def block(side, k):
        return side * (nblk - 1) + k * (1 - 2 * side)

    def beyond(side, k):
        return side * (nblk + 1 + 2 * k) - 1 - k

    def remote(src, dst, here, there, side):
        return pltpu.make_async_remote_copy(
            src_ref=src,
            dst_ref=dst,
            send_sem=send_sem.at[here],
            recv_sem=recv_sem.at[there],
            device_id=(lax.rem(me + n - 1 + 2 * side, n),),
            device_id_type=MESH,
        )

    piece = tile // SPLIT

    def span(h):
        return pl.ds(h * piece, piece)

    def send_p(t, side, k, h):
        here, there = side * REACH + k, (1 - side) * REACH + k
        src, dst = basis.at[t, block(side, k), span(h)], halo.at[there, span(h)]
        remote(src, dst, here * SPLIT + h, there * SPLIT + h, side).start()

    def wait_p(t, side, k):
        here = side * REACH + k
        for h in range(SPLIT):
            src, dst = basis.at[t, block(side, k), span(h)], halo.at[here, span(h)]
            remote(src, dst, here * SPLIT + h, here * SPLIT + h, side).wait()

    more = 2 * REACH * SPLIT

    def send_part(side, k, h):
        here, there = side * REACH + k, (1 - side) * REACH + k
        src, dst = give.at[here, span(h)], got.at[there, span(h)]
        remote(src, dst, more + here * SPLIT + h, more + there * SPLIT + h, side).start()

    def wait_part(side, k, h):
        here = side * REACH + k
        sem = more + here * SPLIT + h
        remote(give.at[here, span(h)], got.at[here, span(h)], sem, sem, side).wait()

    def sum_step(outer, b):
        k = outer * levels + b
        return pltpu.make_async_remote_copy(
            src_ref=sums.at[outer * (levels + 1) + b],
            dst_ref=heard.at[k],
            send_sem=sum_send.at[k],
            recv_sem=sum_recv.at[k],
            device_id=(partners[b],),
            device_id_type=MESH,
        )

    def source(i, d):
        index = nblk * slots
        for k in range(slots):
            index = jnp.where(off_ref[i, k] == d, i * slots + k, index)
        return index

    gram[...] = jnp.zeros_like(gram)
    parts[nblk * slots] = jnp.zeros((tile, probes), F32)

    load_start.wait()
    pl.semaphore_wait(barrier, 2 + levels)
    for k in range(REACH):
        for h in range(SPLIT):
            send_p(0, slow, k, h)
            send_p(0, fast, k, h)
    load_tiles.wait()

    def prepare(i, carry):
        for k in range(slots):
            value = raw[i, k]
            high, low = halves(value)
            fwd[i, pl.ds(0, tile), pl.ds(k * tile, tile)] = high
            fwd[i, pl.ds(tile, tile), pl.ds(k * tile, tile)] = low
            high, low = halves(value.T)
            adj[i, pl.ds(2 * k * tile, tile), :] = high
            adj[i, pl.ds((2 * k + 1) * tile, tile), :] = low
        return carry

    lax.fori_loop(0, nblk, prepare, 0)

    def keep(ref, i, value):
        high, low = halves(value)
        ref[i, :, pl.ds(0, probes)] = high
        ref[i, :, pl.ds(probes, probes)] = low

    def joined(r, base):
        top = r[base : base + tile]
        low = r[base + tile : base + 2 * tile]
        return (top[:, :probes] + top[:, probes:]) + (low[:, :probes] + low[:, probes:])

    def gram_rows(t):
        def one(u, carry):
            prod = (basis[t] * basis[u]).reshape(-1, probes)
            s = jnp.sum(prod.reshape(-1, 8, probes), axis=0)
            gram[pl.ds(t * 2 * DEPTH + u, 1), :] = jnp.sum(s, axis=0, keepdims=True)
            return carry

        lax.fori_loop(0, t + 1, one, 0)

    def forward(t, i):
        rhs = jnp.concatenate([field[i + REACH + off_ref[i, k]] for k in range(slots)], axis=0)
        q = joined(jnp.dot(fwd[i], rhs, preferred_element_type=F32), 0)
        basis[t + 1, i] = q
        keep(image, i, q)
        r = jnp.dot(adj[i], image[i], preferred_element_type=F32)
        for k in range(slots):
            parts[i * slots + k] = joined(r, 2 * k * tile)

    def arrive(t, side, k):
        wait_p(t, side, k)
        keep(field, beyond(side, k) + REACH, halo[side * REACH + k])

    def hand_over(side):
        for k in range(REACH):
            for h in range(SPLIT):
                total = None
                for r in range(REACH - k):
                    index = source(block(side, r), (2 * side - 1) * (r + 1 + k))
                    term = parts[index, span(h)]
                    total = term if total is None else total + term
                give[side * REACH + k, span(h)] = total
                send_part(side, k, h)

    def gathered(target):
        total = None
        for i in range(nblk):
            if abs(target - i) <= REACH:
                term = parts[source(i, target - i)]
                total = term if total is None else total + term
        return total

    def take(t, side, k, last):
        for h in range(SPLIT):
            wait_part(side, k, h)
            basis[t, block(side, k), span(h)] += got[side * REACH + k, span(h)]
            if not last:
                send_p(t, side, k, h)

    def pair(outer, j, last):
        t = 2 * j
        for i in range(nblk):
            keep(field, i + REACH, basis[t, i])
        gram_rows(t)
        for k in range(REACH):
            arrive(t, fast, k)
        for i in range(REACH, nblk - REACH):
            forward(t, i)
        for k in reversed(range(REACH)):
            forward(t, block(fast, k))
        hand_over(fast)
        for k in range(REACH):
            arrive(t, slow, k)
            forward(t, block(slow, REACH - 1 - k))
        hand_over(slow)
        if last:
            gram_rows(t + 1)
            sums[outer * (levels + 1)] = gram[...]
            sum_step(outer, 0).start()
        for i in range(nblk):
            basis[t + 2, i] = gathered(i)
        for k in range(REACH):
            take(t + 2, fast, k, last)
        if last:
            for b in range(levels):
                sum_step(outer, b).wait()
                k = outer * (levels + 1) + b
                sums[k + 1] = sums[k] + heard[outer * levels + b]
                if b + 1 < levels:
                    sum_step(outer, b + 1).start()
        else:
            gram_rows(t + 1)
        for k in range(REACH):
            take(t + 2, slow, k, last)

    def outer_step(outer, carry):
        def inner(j, c):
            pair(outer, j, False)
            return c

        lax.fori_loop(0, DEPTH - 1, inner, 0)
        pair(outer, DEPTH - 1, True)
        total = outer * (levels + 1) + levels
        size = 2 * DEPTH
        corner = sums[total, pl.ds(size * size - 1, 1), :] / total_rows
        scale = 1.0 / jnp.sqrt(corner + 0.25)
        basis[0] = basis[size] * scale[None]

        @pl.when(outer < OUTER - 1)
        def _():
            for k in range(REACH):
                for h in range(SPLIT):
                    send_p(0, slow, k, h)
                    send_p(0, fast, k, h)

        when = [2 * a for a in range(DEPTH)] + [2 * a + 1 for a in range(DEPTH)]
        for a in range(size):
            for b in range(size):
                row = max(when[a], when[b]) * size + min(when[a], when[b])
                gram_ref[outer, pl.ds(a * size + b, 1), :] = (
                    sums[total, pl.ds(row, 1), :] / total_rows
                )
        return carry

    lax.fori_loop(0, OUTER, outer_step, 0)
    final_ref[...] = basis[0]


def on_device(tiles, offsets, start):
    n = lax.axis_size("blk")
    levels = n.bit_length() - 1
    assert n == 1 << levels
    nblk, slots, tile, _ = tiles.shape
    rows, probes = start.shape
    assert nblk >= 2 * REACH
    size = 2 * DEPTH
    dma = pltpu.SemaphoreType.DMA
    grams, final = pl.pallas_call(
        functools.partial(kernel, n, levels, float(rows * n)),
        out_shape=(
            jax.ShapeDtypeStruct((OUTER, size * size, probes), F32),
            jax.ShapeDtypeStruct((nblk, tile, probes), F32),
        ),
        in_specs=[
            pl.BlockSpec(memory_space=pltpu.SMEM),
            pl.BlockSpec(memory_space=pl.ANY),
            pl.BlockSpec(memory_space=pl.ANY),
        ],
        out_specs=(pl.BlockSpec(memory_space=pltpu.VMEM), pl.BlockSpec(memory_space=pltpu.VMEM)),
        scratch_shapes=[
            pltpu.VMEM(tiles.shape, F32),
            pltpu.VMEM((nblk, 2 * tile, slots * tile), BF16),
            pltpu.VMEM((nblk, 2 * slots * tile, tile), BF16),
            pltpu.VMEM((size + 1, nblk, tile, probes), F32),
            pltpu.VMEM((nblk + 2 * REACH, tile, 2 * probes), BF16),
            pltpu.VMEM((nblk, tile, 2 * probes), BF16),
            pltpu.VMEM((nblk * slots + 1, tile, probes), F32),
        ]
        + [pltpu.VMEM((2 * REACH, tile, probes), F32)] * 3
        + [
            pltpu.VMEM((size * size, probes), F32),
            pltpu.VMEM((OUTER * (levels + 1), size * size, probes), F32),
            pltpu.VMEM((OUTER * levels, size * size, probes), F32),
            dma((2,)),
            dma((4 * REACH * SPLIT,)),
            dma((4 * REACH * SPLIT,)),
            dma((OUTER * levels,)),
            dma((OUTER * levels,)),
        ],
        compiler_params=pltpu.CompilerParams(collective_id=0, has_side_effects=True),
    )(offsets, tiles, start.reshape(nblk, tile, probes))
    return grams.reshape(OUTER, size, size, probes), final.reshape(rows, probes)


def solution(mesh):
    placed = (P("blk", None, None, None), P("blk", None), P("blk", None))
    return jax.shard_map(
        on_device, mesh=mesh, in_specs=placed, out_specs=(P(), P("blk", None)), check_vma=False
    )
```
